32 devices in a mesh: pts: 16 (over z, x, core), grp: 2 (over y).
Axes of the slice: x: 2, y: 2, z: 4, core: 2. Of those that a mesh axis runs over, the one named last changes fastest.
Arguments:
- cam_jac: float32 [2, 9, 219136], P(None, None, ('pts', 'grp')), may hold values from -6 to 6
- pt_jac: float32 [2, 3, 219136], P(None, None, ('pts', 'grp')), may hold values from -6 to 6
- cam_slot: int32 [219136], P(('pts', 'grp')), may hold values from 0 to 127
- obs_point: int32 [219136], P(('pts', 'grp')), may hold values from 0 to 2047
- cam_inverse: float32 [9, 9, 13696], replicated, may hold values from -1 to 1, as said below
- pt_inverse: float32 [3, 3, 65536], P(None, None, ('pts', 'grp')), may hold values from -1 to 1, as said below
- cam_rhs: float32 [9, 13696], replicated, may hold values from -48 to 48
- pt_rhs: float32 [3, 65536], P(None, ('pts', 'grp')), may hold values from -240 to 240
Outputs:
- camera_step: float32 [9, 13696], replicated
- point_step: float32 [3, 65536], P(None, ('pts', 'grp'))
- resid_ratio: float32 [], replicated
The draws below stay inside these ranges and needn't reach their ends.
Inputs may be any that keep to these rules, and one draw needn't show every extreme that they name: The observations of each device come in 107 runs of 64; run b holds observations of cameras b * 128 to (b + 1) * 128 - 1, and cam_slot is the camera's offset in that run's block. The point of observation o is (o // 6848) * 2048 + obs_point[o]. `cam_inverse`: each camera's 9 x 9 block is symmetric positive definite. `pt_inverse`: each point's 3 x 3 block is symmetric positive definite.
All inputs are finite; a program needn't handle non-finite values.
Results may differ from the reference program's by a relative error of at most 0.00014.
Values sent between devices are 32-bit elements; how exact they have to be, the bound alone decides.
A program may use at most 128 MiB of HBM per device.

```python
import math
import jax
import jax.numpy as jnp
from jax import lax

CAM_BLK = 128
CAMS = 13696
SLOTS = 64
PTS_DEV = 2048
TERMS = 3
OBS_DEV = 6848
OBS = 219136
PTS = 65536
CAM_OBS = 16


def spd_blocks(key, order, count, low, high, coupling):
    key_scale, key_offdiag = jax.random.split(key)
    scales = jnp.exp(jax.random.uniform(key_scale, (order, count), jnp.float32, math.log(low), math.log(high)))
    offdiag = jax.random.uniform(key_offdiag, (order, order, count), jnp.float32, -coupling, coupling)
    offdiag = 0.5 * (offdiag + jnp.transpose(offdiag, (1, 0, 2)))
    identity = jnp.eye(order, dtype=jnp.float32)[:, :, None]
    coupled = identity + offdiag * (1.0 - identity)
    roots = jnp.sqrt(scales)
    return roots[:, None, :] * coupled * roots[None, :, :]


def draw_cam_inverse(key, part):
    return spd_blocks(key, 9, CAMS, 0.4 / CAM_OBS, 1.6 / CAM_OBS, 0.11)


def draw_pt_inverse(key, part):
    return spd_blocks(key, 3, PTS, 0.03, 0.3, 0.4)


def draw_pt_rhs(key, part):
    ramp = jnp.arange(PTS, dtype=jnp.float32) / PTS
    noise = jnp.clip(jax.random.normal(key, (3, PTS), jnp.float32), -5.0, 5.0)
    return 16.0 * noise * (1.0 + 2.0 * ramp)[None, :]


def place_ends(drawn, stream_key, least, high):
    dims = drawn.shape
    spot = [jax.random.randint(jax.random.fold_in(stream_key, axis), (), 0, dims[axis]) for axis in range(len(dims))]
    drawn = drawn.at[tuple(spot)].set(least)
    longest = dims.index(max(dims))
    spot[longest] = (spot[longest] + 1) % dims[longest]
    return drawn.at[tuple(spot)].set(high)


def block_scale(stream_key, extent, cuts, low, top_value):
    loudness, own = 1.0, jax.random.fold_in(stream_key, 6)
    for dim, shards_of in cuts:
        steps = jnp.exp(jax.random.uniform(jax.random.fold_in(own, dim), (shards_of,), jnp.float32, low / len(cuts), top_value / len(cuts)))
        loudness = loudness * jnp.repeat(steps, extent[dim] // shards_of).reshape([-1 if axis == dim else 1 for axis in range(len(extent))])
    return loudness


def scatter_about(key, extent, width, reach, cuts=(), kind=jnp.bfloat16):
    array = jax.random.normal(key, extent, jnp.float32) * width
    if len(cuts) > 0:
        array = block_scale(key, extent, cuts, -0.22, 0.18) * array
    return jnp.clip(array, min=-reach, max=reach).astype(kind)


def setup_inputs(seed: int = 0) -> dict:
    seeds = jax.random.split(jax.random.key(seed), 9)
    return {
        "cam_jac": scatter_about(seeds[0], (2, 9, OBS), 1.0, 6.0, ((2, 32),), jnp.float32),
        "pt_jac": scatter_about(seeds[1], (2, 3, OBS), 1.0, 6.0, ((2, 32),), jnp.float32),
        "cam_slot": place_ends(jax.random.randint(seeds[2], (OBS,), 0, CAM_BLK), jax.random.fold_in(seeds[2], 1), 0, CAM_BLK - 1).astype(jnp.int32),
        "obs_point": place_ends(jax.random.randint(seeds[3], (OBS,), 0, PTS_DEV), jax.random.fold_in(seeds[3], 1), 0, PTS_DEV - 1).astype(jnp.int32),
        "cam_inverse": draw_cam_inverse(jax.random.fold_in(seeds[8], 71), 0),
        "pt_inverse": draw_pt_inverse(jax.random.fold_in(seeds[8], 71), 0),
        "cam_rhs": scatter_about(seeds[6], (9, CAMS), (0.5 * CAM_OBS), 48.0, (), jnp.float32),
        "pt_rhs": draw_pt_rhs(jax.random.fold_in(seeds[8], 71), 0),
    }


def reference(cam_jac, pt_jac, cam_slot, obs_point, cam_inverse, pt_inverse, cam_rhs, pt_rhs):
    total = cam_slot.shape[0]
    cameras = cam_rhs.shape[1]
    points = pt_rhs.shape[1]
    positions = jnp.arange(total, dtype=jnp.int32)
    cam_index = positions % OBS_DEV // SLOTS * CAM_BLK + cam_slot
    pt_index = positions // OBS_DEV * PTS_DEV + obs_point

    def to_points(camera_vec):
        at_obs = camera_vec[:, cam_index]
        projected = lax.optimization_barrier(jnp.sum(cam_jac * at_obs[None], axis=1))
        lifted = lax.optimization_barrier(jnp.sum(pt_jac * projected[:, None], axis=0))
        return jnp.zeros((3, points), jnp.float32).at[:, pt_index].add(lifted)

    def to_cameras(point_vec):
        at_obs = point_vec[:, pt_index]
        projected = lax.optimization_barrier(jnp.sum(pt_jac * at_obs[None], axis=1))
        pulled = lax.optimization_barrier(jnp.sum(cam_jac * projected[:, None], axis=0))
        return jnp.zeros((9, cameras), jnp.float32).at[:, cam_index].add(pulled)

    def point_solve(point_vec):
        return lax.optimization_barrier(jnp.sum(pt_inverse * point_vec[None], axis=1))

    def camera_solve(camera_vec):
        return lax.optimization_barrier(jnp.sum(cam_inverse * camera_vec[None], axis=1))
    reduced = cam_rhs - to_cameras(point_solve(pt_rhs))
    series_term = camera_solve(reduced)
    camera_step = series_term
    for series_index in range(TERMS):
        series_term = camera_solve(to_cameras(point_solve(to_points(series_term))))
        camera_step = camera_step + series_term
    point_resid = pt_rhs - to_points(camera_step)
    point_step = point_solve(point_resid)
    resid_ratio = jnp.sqrt(jnp.sum(point_resid * point_resid) / jnp.sum(pt_rhs * pt_rhs))
    return (camera_step, point_step, resid_ratio)
```

```python
import functools

import jax
import jax.numpy as jnp
from jax import lax
from jax.experimental import pallas as pl
from jax.experimental.pallas import tpu as pltpu
from jax.sharding import PartitionSpec as P

CAM_BLK = 128
TERMS = 3
PER = 4
ROWS = 40
MESH = pl.DeviceIdType.MESH
VMEM = pl.BlockSpec(memory_space=pltpu.VMEM)
F32 = jnp.float32
BF16 = jnp.bfloat16


def halves(v):
    top = v.astype(BF16)
    return top, (v - top.astype(F32)).astype(BF16)


def rows_of(group):
    return pl.ds(16 * (group // 2) + group % 2, 8, stride=2)


def to_points(live, groups, vec, cj, pj, slot, point, quant, left, right):
    lane_low = lax.broadcasted_iota(jnp.int32, (8, 128), 1) < 64
    for group in range(groups):
        u, half = group // 2, group % 2
        rows = rows_of(group)
        index = slot[rows, :]
        proj = [None, None]
        for j in range(9):
            even = vec[pl.ds(8 * u * ROWS + (2 * half) * 9 + j, 8, stride=ROWS), :]
            odd = vec[pl.ds(8 * u * ROWS + (2 * half + 1) * 9 + j, 8, stride=ROWS), :]
            even = jnp.take_along_axis(even, index, axis=1, mode="promise_in_bounds")
            odd = jnp.take_along_axis(odd, index, axis=1, mode="promise_in_bounds")
            got = jnp.where(lane_low, even, odd)
            for a in range(2):
                part = cj[a * 9 + j, rows, :] * got
                proj[a] = part if proj[a] is None else proj[a] + part
        for i in range(3):
            quant[i, rows, :] = pj[i, rows, :] * proj[0] + pj[3 + i, rows, :] * proj[1]
    low = lax.broadcasted_iota(jnp.int32, (128, 128), 0)
    high = lax.broadcasted_iota(jnp.int32, (16, 128), 0)
    for r in range(live):
        cols = slice(r * 128, (r + 1) * 128)
        where = point[r : r + 1, :]
        right[:, cols] = jnp.where(low == (where & 127), 1.0, 0.0).astype(BF16)
        hit = high == (where >> 7)
        for i in range(3):
            v = jnp.where(hit, quant[i, r : r + 1, :], 0.0)
            top, rest = halves(v)
            left[i * 16 : i * 16 + 16, cols] = top
            left[48 + i * 16 : 64 + i * 16, cols] = rest
    both = lax.dot_general(
        left[:, : live * 128], right[:, : live * 128], (((1,), (1,)), ((), ())), preferred_element_type=F32
    )
    return [both[i * 16 : i * 16 + 16] + both[48 + i * 16 : 64 + i * 16] for i in range(3)]


def point_solve(pinv, y):
    return [
        pinv[3 * i] * y[0] + pinv[3 * i + 1] * y[1] + pinv[3 * i + 2] * y[2] for i in range(3)
    ]


def to_cameras(live, groups, z, cj, pj, slot, point, pull, out):
    for group in range(groups):
        rows = rows_of(group)
        where = point[rows, :]
        low, high = where & 127, where >> 7
        got = [jnp.zeros((8, 128), F32)] * 3
        for s in range(16):
            hit = high == s
            for i in range(3):
                row = jnp.broadcast_to(z[i][s : s + 1, :], (8, 128))
                cand = jnp.take_along_axis(row, low, axis=1, mode="promise_in_bounds")
                got[i] = jnp.where(hit, cand, got[i])
        proj = [
            pj[3 * a, rows, :] * got[0] + pj[3 * a + 1, rows, :] * got[1] + pj[3 * a + 2, rows, :] * got[2]
            for a in range(2)
        ]
        for j in range(9):
            pull[pl.ds(64 * j + 16 * (group // 2) + group % 2, 8, stride=2), :] = (
                cj[j, rows, :] * proj[0] + cj[9 + j, rows, :] * proj[1]
            )
    pull[pl.ds(9 * 64, 7 * 64), :] = jnp.zeros((7 * 64, 128), F32)
    lane_low = lax.broadcasted_iota(jnp.int32, (16, 128), 1) < 64
    cams = lax.broadcasted_iota(jnp.int32, (128, 128), 0)
    for r in range(live):
        v = pull[pl.ds(r, 16, stride=64), :]
        e_top, e_rest = halves(jnp.where(lane_low, v, 0.0))
        o_top, o_rest = halves(jnp.where(lane_low, 0.0, v))
        lhs = jnp.concatenate([e_top, e_rest, o_top, o_rest], axis=0)
        hot = jnp.where(cams == slot[r : r + 1, :], 1.0, 0.0).astype(BF16)
        d = lax.dot_general(lhs, hot, (((1,), (1,)), ((), ())), preferred_element_type=F32)
        base = (r // 2) * ROWS + (r % 2) * 18
        out[base : base + 9, :] = (d[0:16] + d[16:32])[0:9]
        out[base + 9 : base + 18, :] = (d[32:48] + d[48:64])[0:9]


def first_body(live, groups, cj, pj, slot, point, pinv, prhs, out, pull):
    z = point_solve(pinv, [prhs[i] for i in range(3)])
    to_cameras(live, groups, z, cj, pj, slot, point, pull, out)


def middle_body(live, groups, vec, cj, pj, slot, point, pinv, out, quant, left, right, pull):
    y = to_points(live, groups, vec, cj, pj, slot, point, quant, left, right)
    z = point_solve(pinv, y)
    to_cameras(live, groups, z, cj, pj, slot, point, pull, out)


def last_body(live, groups, vec, cj, pj, slot, point, pinv, prhs, step, sums, quant, left, right):
    y = to_points(live, groups, vec, cj, pj, slot, point, quant, left, right)
    rhs = [prhs[i] for i in range(3)]
    resid = [rhs[i] - y[i] for i in range(3)]
    z = point_solve(pinv, resid)
    for i in range(3):
        step[i] = z[i]
    for row, vals in ((0, resid), (1, rhs)):
        total = vals[0] * vals[0] + vals[1] * vals[1] + vals[2] * vals[2]
        sums[8 * row : 8 * row + 8, :] = total[0:8] + total[8:16]


def place(grp_size):
    pts, grp = lax.axis_index("pts"), lax.axis_index("grp")
    core = lax.rem(pts, 2)
    chip = (pts // 2) * grp_size + grp

    def at(other):
        return (2 * (other // grp_size) + core, lax.rem(other, grp_size))

    return core, chip, at, (pts + 1 - 2 * core, grp)


def greet(chips, chip, at, twin):
    barrier = pltpu.get_barrier_semaphore()
    pl.semaphore_signal(barrier, inc=1, device_id=twin, device_id_type=MESH)

    def say(k, _):
        pl.semaphore_signal(barrier, inc=1, device_id=at(lax.rem(chip + k, chips)), device_id_type=MESH)
        return 0

    lax.fori_loop(1, chips, say, 0)
    pl.semaphore_wait(barrier, chips)


def combine_body(
    chips, grp_size, chunks, slots, mode, x, inv, base, out, kept,
    twin_buf, mine, inbox, result, a_s, a_r, b_s, b_r, c_s, c_r, d_s, d_r,
):
    core, chip, at, twin = place(grp_size)
    greet(chips, chip, at, twin)

    def owned(c, t):
        return jnp.logical_and(t < slots, c * slots + t < chunks)

    def remote(src, dst, send, recv, device):
        return pltpu.make_async_remote_copy(
            src_ref=src, dst_ref=dst, send_sem=send, recv_sem=recv, device_id=device, device_id_type=MESH
        )

    def loop(start, body):
        def step(k, carry):
            body(k)
            return carry

        lax.fori_loop(start, chips, step, 0)

    def around(k):
        return lax.rem(chip + k, chips)

    def to_twin(t):
        return remote(x.at[1 - core, t], twin_buf.at[t], a_s.at[t], a_r.at[t], twin)

    def to_owner(t):
        return remote(mine.at[t], inbox.at[chip], b_s.at[t], b_r.at[chip], at(t))

    def from_peer(t):
        return remote(mine.at[0], inbox.at[t], b_s.at[0], b_r.at[t], at(t))

    def spread(t):
        return remote(result.at[core, chip], result.at[core, chip], c_s.at[t], c_r.at[chip], at(t))

    def spread_in(t):
        return remote(result.at[core, t], result.at[core, t], c_s.at[0], c_r.at[t], at(t))

    def pass_on(t):
        return remote(result.at[core, t], result.at[core, t], d_s.at[t], d_r.at[t], twin)

    def pass_in(t):
        return remote(result.at[1 - core, t], result.at[1 - core, t], d_s.at[0], d_r.at[t], twin)

    def start_twin(k):
        t = around(k)
        pl.when(owned(1 - core, t))(lambda: to_twin(t).start())

    loop(1, start_twin)
    start_twin(0)

    def reduce_pair(k, send):
        t = around(k)

        @pl.when(owned(core, t))
        def _():
            to_twin(t).wait_recv()
            mine[t] = x[core, t] + twin_buf[t]
            if send:
                to_owner(t).start()

    loop(1, lambda k: reduce_pair(k, True))
    reduce_pair(0, False)

    @pl.when(owned(core, chip))
    def _():
        kept[...] = mine[chip]

        def gather(k):
            t = around(k)
            from_peer(t).wait_recv()
            kept[...] += inbox[t]

        loop(1, gather)
        total = base[...] - kept[...] if mode == 0 else kept[...]
        solved = []
        for b in range(PER):
            piece = None
            for j in range(9):
                term = inv[b, j] * total[9 * b + j : 9 * b + j + 1, :]
                piece = term if piece is None else piece + term
            solved.append(piece)
        solved = jnp.concatenate(solved + [jnp.zeros((ROWS - 9 * PER, 128), F32)], axis=0)
        kept[...] = solved if mode == 0 else solved + base[...]
        result[core, chip] = solved if mode < 2 else solved + base[...]
        loop(1, lambda k: spread(around(k)).start())
        pass_on(chip).start()

    @pl.when(jnp.logical_not(owned(core, chip)))
    def _():
        kept[...] = jnp.zeros((ROWS, 128), F32)

    def forward(k):
        t = around(chips - k)

        @pl.when(owned(core, t))
        def _():
            spread_in(t).wait_recv()
            pass_on(t).start()

    loop(1, forward)

    def finish(k):
        t = around(k)
        pl.when(owned(1 - core, t))(lambda: pass_in(t).wait_recv())

    loop(0, finish)
    for c in range(2):
        for t in range(slots):
            if c * slots + t < chunks:
                out[c, t] = result[c, t]
            else:
                out[c, t] = jnp.zeros((ROWS, 128), F32)

    def drain(k):
        t = around(k)
        pl.when(owned(1 - core, t))(lambda: to_twin(t).wait_send())
        pl.when(owned(core, t))(lambda: pass_on(t).wait_send())

    loop(0, drain)

    def drain_peers(k):
        t = around(k)
        pl.when(owned(core, t))(lambda: to_owner(t).wait_send())
        pl.when(owned(core, chip))(lambda: spread(t).wait_send())

    loop(1, drain_peers)


def ratio_body(chips, grp_size, sums, out, pair, inbox, twin_s, twin_r, b_s, b_r):
    core, chip, at, twin = place(grp_size)
    greet(chips, chip, at, twin)

    def send_twin():
        return pltpu.make_async_remote_copy(
            src_ref=sums, dst_ref=pair, send_sem=twin_s, recv_sem=twin_r, device_id=twin, device_id_type=MESH
        )

    def send(t, slot):
        return pltpu.make_async_remote_copy(
            src_ref=inbox.at[chip], dst_ref=inbox.at[slot], send_sem=b_s.at[t], recv_sem=b_r.at[slot],
            device_id=at(t), device_id_type=MESH,
        )

    send_twin().start()
    send_twin().wait_recv()
    inbox[chip] = sums[...] + pair[...]

    def begin(k, carry):
        send(lax.rem(chip + k, chips), chip).start()
        return carry

    def end(k, carry):
        t = lax.rem(chip + k, chips)
        send(t, t).wait_recv()
        return carry

    def drain(k, carry):
        send(lax.rem(chip + k, chips), chip).wait_send()
        return carry

    lax.fori_loop(1, chips, begin, 0)
    lax.fori_loop(1, chips, end, 0)
    total = inbox[0]
    for t in range(1, chips):
        total = total + inbox[t]
    resid = jnp.sum(total[0:8], keepdims=True)
    rhs = jnp.sum(total[8:16], keepdims=True)
    out[...] = jnp.broadcast_to(jnp.sqrt(resid / rhs), (8, 128))
    lax.fori_loop(1, chips, drain, 0)
    send_twin().wait_send()


def local(pts_size, grp_size, cam_jac, pt_jac, cam_slot, obs_point, cam_inverse, pt_inverse, cam_rhs, pt_rhs):
    obs_count = cam_slot.shape[0]
    cameras = cam_rhs.shape[1]
    blocks = cameras // CAM_BLK
    points = pt_rhs.shape[1]
    chips = pts_size * grp_size // 2
    chunks = -(-blocks // PER)
    slots = -(-chunks // 16) * 8
    assert obs_count == blocks * 64 and slots <= chips and slots == 16 and points == 2048
    width = slots * 2 * 2 * 128
    live = -(-obs_count // 128)
    groups = 2 * (-(-live // 16))
    chunk_cams = PER * CAM_BLK

    def pad_obs(v):
        lead = v.shape[:-1]
        v = jnp.pad(v, [(0, 0)] * len(lead) + [(0, width - obs_count)])
        return v.reshape(-1, width // 128, 128)

    cj, pj = pad_obs(cam_jac), pad_obs(pt_jac)
    slot, point = pad_obs(cam_slot)[0], pad_obs(obs_point)[0]
    pinv = pt_inverse.reshape(9, 16, 128)
    prhs = pt_rhs.reshape(3, 16, 128)

    pts, grp = lax.axis_index("pts"), lax.axis_index("grp")
    chunk = (pts % 2) * slots + (pts // 2) * grp_size + grp
    begin = jnp.minimum(chunk * chunk_cams, cameras)
    edge = jnp.minimum(begin, cameras - chunk_cams)

    def own(v):
        part = lax.dynamic_slice_in_dim(v, edge, chunk_cams, axis=v.ndim - 1)
        part = jnp.pad(part, [(0, 0)] * (v.ndim - 1) + [(0, chunk_cams)])
        part = lax.dynamic_slice_in_dim(part, begin - edge, chunk_cams, axis=v.ndim - 1)
        return part.reshape(v.shape[:-1] + (PER, CAM_BLK))

    inv = jnp.transpose(own(cam_inverse), (2, 1, 0, 3))
    rhs = jnp.transpose(own(cam_rhs), (1, 0, 2)).reshape(PER * 9, 128)
    rhs = jnp.pad(rhs, ((0, ROWS - PER * 9), (0, 0)))

    vec_shape = jax.ShapeDtypeStruct((2 * slots * ROWS, 128), F32)
    quant = pltpu.VMEM((3, width // 128, 128), F32)
    left = pltpu.VMEM((96, width), BF16)
    right = pltpu.VMEM((128, width), BF16)
    pull = pltpu.VMEM((16 * 64, 128), F32)

    first = pl.pallas_call(
        functools.partial(first_body, live, groups),
        out_shape=vec_shape, in_specs=[VMEM] * 6, out_specs=VMEM, scratch_shapes=[pull], name="first",
    )
    middle = pl.pallas_call(
        functools.partial(middle_body, live, groups),
        out_shape=vec_shape, in_specs=[VMEM] * 6, out_specs=VMEM,
        scratch_shapes=[quant, left, right, pull], name="middle",
    )
    last = pl.pallas_call(
        functools.partial(last_body, live, groups),
        out_shape=(jax.ShapeDtypeStruct((3, 16, 128), F32), jax.ShapeDtypeStruct((16, 128), F32)),
        in_specs=[VMEM] * 7, out_specs=(VMEM, VMEM), scratch_shapes=[quant, left, right], name="last",
    )

    def combine(mode, x, base):
        dma = pltpu.SemaphoreType.DMA
        full, kept = pl.pallas_call(
            functools.partial(combine_body, chips, grp_size, chunks, slots, mode),
            out_shape=(
                jax.ShapeDtypeStruct((2, slots, ROWS, 128), F32),
                jax.ShapeDtypeStruct((ROWS, 128), F32),
            ),
            in_specs=[VMEM] * 3, out_specs=(VMEM, VMEM),
            scratch_shapes=[
                pltpu.VMEM((slots, ROWS, 128), F32),
                pltpu.VMEM((slots, ROWS, 128), F32),
                pltpu.VMEM((chips, ROWS, 128), F32),
                pltpu.VMEM((2, slots, ROWS, 128), F32),
                dma((slots,)), dma((slots,)), dma((slots,)), dma((chips,)),
                dma((chips,)), dma((slots,)), dma((slots,)), dma((slots,)),
            ],
            compiler_params=pltpu.CompilerParams(collective_id=mode, has_side_effects=True),
            name=f"combine{mode}",
        )(x.reshape(2, slots, ROWS, 128), inv, base)
        return full.reshape(2 * slots * ROWS, 128), kept

    vec, kept = combine(0, first(cj, pj, slot, point, pinv, prhs), rhs)
    for index in range(TERMS):
        x = middle(vec, cj, pj, slot, point, pinv)
        vec, kept = combine(2 if index == TERMS - 1 else 1, x, kept)
    step, sums = last(vec, cj, pj, slot, point, pinv, prhs)
    dma = pltpu.SemaphoreType.DMA
    ratio = pl.pallas_call(
        functools.partial(ratio_body, chips, grp_size),
        out_shape=jax.ShapeDtypeStruct((8, 128), F32), in_specs=[VMEM], out_specs=VMEM,
        scratch_shapes=[
            pltpu.VMEM((16, 128), F32), pltpu.VMEM((chips, 16, 128), F32),
            dma, dma, dma((chips,)), dma((chips,)),
        ],
        compiler_params=pltpu.CompilerParams(collective_id=3, has_side_effects=True),
        name="ratio",
    )(sums)
    camera_step = vec.reshape(2 * slots, ROWS, 128)[:, : PER * 9].reshape(2 * slots * PER, 9, 128)
    camera_step = jnp.transpose(camera_step[:blocks], (1, 0, 2)).reshape(9, cameras)
    return camera_step, step.reshape(3, points), ratio[0, 0]


def solution(mesh):
    placed = (
        P(None, None, ("pts", "grp")),
        P(None, None, ("pts", "grp")),
        P(("pts", "grp")),
        P(("pts", "grp")),
        P(),
        P(None, None, ("pts", "grp")),
        P(),
        P(None, ("pts", "grp")),
    )
    return jax.shard_map(
        functools.partial(local, mesh.shape["pts"], mesh.shape["grp"]),
        mesh=mesh,
        in_specs=placed,
        out_specs=(P(), P(None, ("pts", "grp")), P()),
        check_vma=False,
    )
```

```python
import functools

import jax
import jax.numpy as jnp
from jax import lax
from jax.experimental import pallas as pl
from jax.experimental.pallas import tpu as pltpu
from jax.sharding import PartitionSpec as P

CAM_BLK = 128
TERMS = 3
PER = 4
ROWS = 40
MESH = pl.DeviceIdType.MESH
VMEM = pl.BlockSpec(memory_space=pltpu.VMEM)
F32 = jnp.float32
BF16 = jnp.bfloat16


def halves(v):
    top = v.astype(BF16)
    return top, (v - top.astype(F32)).astype(BF16)


def rows_of(group):
    return 16 * (group // 2) + group % 2


def prepare(obs, live, cj_in, pj_in, slot, point, pinv_in, prhs_in, cj, pj, pinv, prhs, tail, right, hot):
    for a in range(2):
        for ref, out, count in ((cj_in, cj, 9), (pj_in, pj, 3)):
            for j in range(count):
                begin = live // 8 * 8
                out[(a * count + j) * 64 + begin : (a * count + j + 1) * 64, :] = jnp.zeros((64 - begin, 128), F32)
    tail[...] = jnp.zeros((16, 128), F32)
    for r in range(live):
        span = min(128, obs - r * 128)
        for a in range(2):
            for ref, out, count in ((cj_in, cj, 9), (pj_in, pj, 3)):
                if span == 128:
                    v = ref[a, :, r * 128 : r * 128 + 128]
                else:
                    tail[0:count, 0:span] = ref[a, :, r * 128 : r * 128 + span]
                    v = tail[0:count, :]
                out[pl.ds(a * count * 64 + r, count, stride=64), :] = v
    for s in range(16):
        cols = slice(s * 128, s * 128 + 128)
        prhs[pl.ds(s, 3, stride=16), :] = prhs_in[:, cols]
        for i in range(3):
            pinv[pl.ds(48 * i + s, 3, stride=16), :] = pinv_in[i, :, cols]
    low = lax.broadcasted_iota(jnp.int32, (128, 128), 0)
    for r in range(live):
        cols = slice(r * 128, (r + 1) * 128)
        right[:, cols] = jnp.where(low == (point[r : r + 1, :] & 127), 1.0, 0.0).astype(BF16)
        hot[:, cols] = jnp.where(low == slot[r : r + 1, :], 1.0, 0.0).astype(BF16)


def to_points(live, groups, vec, cj, pj, slot, point, quant, left, right):
    lane_low = lax.broadcasted_iota(jnp.int32, (8, 128), 1) < 64
    for group in range(groups):
        u, half = group // 2, group % 2
        row = rows_of(group)
        index = slot[pl.ds(row, 8, stride=2), :]
        proj = [None, None]
        for j in range(9):
            even = vec[pl.ds(8 * u * ROWS + (2 * half) * 9 + j, 8, stride=ROWS), :]
            odd = vec[pl.ds(8 * u * ROWS + (2 * half + 1) * 9 + j, 8, stride=ROWS), :]
            even = jnp.take_along_axis(even, index, axis=1, mode="promise_in_bounds")
            odd = jnp.take_along_axis(odd, index, axis=1, mode="promise_in_bounds")
            got = jnp.where(lane_low, even, odd)
            for a in range(2):
                part = cj[pl.ds((a * 9 + j) * 64 + row, 8, stride=2), :] * got
                proj[a] = part if proj[a] is None else proj[a] + part
        for i in range(3):
            quant[pl.ds(64 * i + row, 8, stride=2), :] = (
                pj[pl.ds(64 * i + row, 8, stride=2), :] * proj[0]
                + pj[pl.ds(64 * (3 + i) + row, 8, stride=2), :] * proj[1]
            )
    high = lax.broadcasted_iota(jnp.int32, (16, 128), 0)
    for r in range(live):
        cols = slice(r * 128, (r + 1) * 128)
        hit = high == (point[r : r + 1, :] >> 7)
        for i in range(3):
            v = jnp.where(hit, quant[64 * i + r : 64 * i + r + 1, :], 0.0)
            top, rest = halves(v)
            left[i * 16 : i * 16 + 16, cols] = top
            left[48 + i * 16 : 64 + i * 16, cols] = rest
    both = lax.dot_general(left[...], right[...], (((1,), (1,)), ((), ())), preferred_element_type=F32)
    return both[0:48] + both[48:96]


def point_solve(pinv, y):
    out = []
    for i in range(3):
        row = 48 * i
        out.append(
            pinv[row : row + 16] * y[0:16] + pinv[row + 16 : row + 32] * y[16:32] + pinv[row + 32 : row + 48] * y[32:48]
        )
    return jnp.concatenate(out, axis=0)


def to_cameras(live, groups, z, cj, pj, slot, point, hot, pull, out):
    for group in range(groups):
        row = rows_of(group)
        where = point[pl.ds(row, 8, stride=2), :]
        low, high = where & 127, where >> 7
        got = [jnp.zeros((8, 128), F32)] * 3
        for s in range(16):
            hit = high == s
            for i in range(3):
                table = jnp.broadcast_to(z[16 * i + s : 16 * i + s + 1, :], (8, 128))
                cand = jnp.take_along_axis(table, low, axis=1, mode="promise_in_bounds")
                got[i] = jnp.where(hit, cand, got[i])
        proj = []
        for a in range(2):
            part = None
            for i in range(3):
                term = pj[pl.ds((3 * a + i) * 64 + row, 8, stride=2), :] * got[i]
                part = term if part is None else part + term
            proj.append(part)
        for j in range(9):
            pull[pl.ds(64 * j + row, 8, stride=2), :] = (
                cj[pl.ds(64 * j + row, 8, stride=2), :] * proj[0]
                + cj[pl.ds(64 * (9 + j) + row, 8, stride=2), :] * proj[1]
            )
    lane_low = lax.broadcasted_iota(jnp.int32, (16, 128), 1) < 64
    for r in range(live):
        v = pull[pl.ds(r, 16, stride=64), :]
        e_top, e_rest = halves(jnp.where(lane_low, v, 0.0))
        o_top, o_rest = halves(jnp.where(lane_low, 0.0, v))
        lhs = jnp.concatenate([e_top, e_rest, o_top, o_rest], axis=0)
        d = lax.dot_general(
            lhs, hot[:, r * 128 : r * 128 + 128], (((1,), (1,)), ((), ())), preferred_element_type=F32
        )
        base = (r // 2) * ROWS + (r % 2) * 18
        out[base : base + 9, :] = (d[0:16] + d[16:32])[0:9]
        out[base + 9 : base + 18, :] = (d[32:48] + d[48:64])[0:9]


def body(
    chips, grp_size, chunks, slots, blocks, live, groups, obs,
    cj_in, pj_in, slot, point, pinv_in, prhs_in, cinv, crhs,
    cam_out, pt_out, ratio_out,
    cj, pj, pinv, prhs, tail, right, hot, left, quant, pull, zs, x, inv, rhs, kept,
    twin_buf, mine, inbox, result, tile, pair, tiles, left_tiles,
    a_s, a_r, b_s, b_r, c_s, c_r, d_s, d_r, load, p_s, p_r, q_s, q_r,
):
    pts, grp = lax.axis_index("pts"), lax.axis_index("grp")
    core = lax.rem(pts, 2)
    chip = (pts // 2) * grp_size + grp
    twin = (pts + 1 - 2 * core, grp)

    def at(other):
        return (2 * (other // grp_size) + core, lax.rem(other, grp_size))

    def around(k):
        return lax.rem(chip + k, chips)

    def loop(start, step):
        def run(k, carry):
            step(k)
            return carry

        lax.fori_loop(start, chips, run, 0)

    barrier = pltpu.get_barrier_semaphore()
    pl.semaphore_signal(barrier, inc=1, device_id=twin, device_id_type=MESH)
    loop(1, lambda k: pl.semaphore_signal(barrier, inc=1, device_id=at(around(k)), device_id_type=MESH))

    def owned(c, t):
        return jnp.logical_and(t < slots, c * slots + t < chunks)

    def owned_block(b):
        return jnp.logical_and(chip < slots, (core * slots + chip) * PER + b < blocks)

    def loads(b):
        cols = pl.ds(pl.multiple_of(((core * slots + chip) * PER + b) * 128, 128), 128)
        return (
            pltpu.make_async_copy(cinv.at[:, :, cols], inv.at[b], load.at[2 * b]),
            pltpu.make_async_copy(crhs.at[:, cols], rhs.at[b], load.at[2 * b + 1]),
        )

    for b in range(PER):
        @pl.when(owned_block(b))
        def _():
            for copy in loads(b):
                copy.start()

        @pl.when(jnp.logical_not(owned_block(b)))
        def _():
            inv[b] = jnp.zeros((9, 9, 128), F32)
            rhs[b] = jnp.zeros((9, 128), F32)

    prepare(obs, live, cj_in, pj_in, slot, point, pinv_in, prhs_in, cj, pj, pinv, prhs, tail, right, hot)
    x[...] = jnp.zeros_like(x)
    result[...] = jnp.zeros_like(result)
    kept[...] = jnp.zeros_like(kept)
    pull[pl.ds(9 * 64, 7 * 64), :] = jnp.zeros((7 * 64, 128), F32)
    zs[...] = prhs[...]
    for b in range(PER):
        @pl.when(owned_block(b))
        def _():
            for copy in loads(b):
                copy.wait()

    pl.semaphore_wait(barrier, chips)

    def chunk(c, t):
        return pl.ds(pl.multiple_of((c * slots + t) * ROWS, 8), ROWS)

    def remote(src, dst, send, recv, device):
        return pltpu.make_async_remote_copy(
            src_ref=src, dst_ref=dst, send_sem=send, recv_sem=recv, device_id=device, device_id_type=MESH
        )

    def to_twin(t):
        return remote(x.at[chunk(1 - core, t)], twin_buf.at[t], a_s.at[t], a_r.at[t], twin)

    def to_owner(t):
        return remote(mine.at[t], inbox.at[chip], b_s.at[t], b_r.at[chip], at(t))

    def from_peer(t):
        return remote(mine.at[0], inbox.at[t], b_s.at[0], b_r.at[t], at(t))

    def spread(t):
        part = result.at[chunk(core, chip)]
        return remote(part, part, c_s.at[t], c_r.at[chip], at(t))

    def spread_in(t):
        part = result.at[chunk(core, t)]
        return remote(part, part, c_s.at[0], c_r.at[t], at(t))

    def pass_on(t):
        part = result.at[chunk(core, t)]
        return remote(part, part, d_s.at[t], d_r.at[t], twin)

    def pass_in(t):
        part = result.at[chunk(1 - core, t)]
        return remote(part, part, d_s.at[0], d_r.at[t], twin)

    def start_twin(k):
        t = around(k)
        pl.when(owned(1 - core, t))(lambda: to_twin(t).start())

    def reduce_pair(k, send):
        t = around(k)

        @pl.when(owned(core, t))
        def _():
            to_twin(t).wait_recv()
            mine[t] = x[chunk(core, t), :] + twin_buf[t]
            if send:
                to_owner(t).start()

    def forward(k):
        t = around(chips - k)

        @pl.when(owned(core, t))
        def _():
            spread_in(t).wait_recv()
            pass_on(t).start()

    def finish(k):
        t = around(k)
        pl.when(owned(1 - core, t))(lambda: pass_in(t).wait_recv())

    def drain(k):
        t = around(k)
        pl.when(owned(1 - core, t))(lambda: to_twin(t).wait_send())
        pl.when(owned(core, t))(lambda: pass_on(t).wait_send())

    def drain_peers(k):
        t = around(k)
        pl.when(owned(core, t))(lambda: to_owner(t).wait_send())
        pl.when(owned(core, chip))(lambda: spread(t).wait_send())

    def exchange(index):
        loop(1, start_twin)
        start_twin(0)
        loop(1, lambda k: reduce_pair(k, True))
        reduce_pair(0, False)

        @pl.when(owned(core, chip))
        def _():
            tile[...] = mine[chip]

            def gather(k):
                t = around(chips - k)
                from_peer(t).wait_recv()
                tile[...] += inbox[t]

            loop(1, gather)
            solved = []
            for b in range(PER):
                total = tile[9 * b : 9 * b + 9, :]
                total = jnp.where(index == 0, rhs[b] - total, total)
                piece = None
                for j in range(9):
                    term = inv[b, j] * total[j : j + 1, :]
                    piece = term if piece is None else piece + term
                solved.append(piece)
            solved = jnp.concatenate(solved + [jnp.zeros((ROWS - 9 * PER, 128), F32)], axis=0)
            step = kept[...] + solved
            kept[...] = step
            result[chunk(core, chip), :] = jnp.where(index == TERMS, step, solved)
            loop(1, lambda k: spread(around(k)).start())
            pass_on(chip).start()

        loop(1, forward)
        loop(0, finish)
        loop(0, drain)
        loop(1, drain_peers)

    def term(index, carry):
        solved = point_solve(pinv, zs[...])
        zs[...] = solved
        to_cameras(live, groups, zs, cj, pj, slot, point, hot, pull, x)
        exchange(index)
        zs[...] = to_points(live, groups, result, cj, pj, slot, point, quant, left, right)
        return carry

    lax.fori_loop(0, TERMS + 1, term, 0)
    rhs_pts = prhs[...]
    resid = rhs_pts - zs[...]
    for row, vals in ((0, resid * resid), (1, rhs_pts * rhs_pts)):
        total = vals[0:8]
        for k in range(1, 6):
            total = total + vals[8 * k : 8 * k + 8]
        tiles[8 * row : 8 * row + 8, :] = total

    def swap():
        return remote(tiles, pair, p_s, p_r, twin)

    def share(t, slot_of):
        return remote(left_tiles.at[chip], left_tiles.at[slot_of], q_s.at[t], q_r.at[slot_of], at(t))

    swap().start()
    swap().wait_recv()
    left_tiles[chip] = tiles[...] + pair[...]
    loop(1, lambda k: share(around(k), chip).start())
    zs[...] = point_solve(pinv, resid)
    for s in range(16):
        pt_out[:, s * 128 : s * 128 + 128] = zs[pl.ds(s, 3, stride=16), :]
    for b in range(blocks):
        base = (b // PER) * ROWS + (b % PER) * 9
        cam_out[:, b * 128 : b * 128 + 128] = result[base : base + 9, :]

    def collect(k):
        t = around(k)
        share(t, t).wait_recv()

    loop(1, collect)
    total = left_tiles[0]
    for t in range(1, chips):
        total = total + left_tiles[t]
    ratio_out[...] = jnp.sqrt(jnp.sum(total[0:8], keepdims=True) / jnp.sum(total[8:16], keepdims=True))
    loop(1, lambda k: share(around(k), chip).wait_send())
    swap().wait_send()


def local(pts_size, grp_size, cam_jac, pt_jac, cam_slot, obs_point, cam_inverse, pt_inverse, cam_rhs, pt_rhs):
    obs = cam_slot.shape[0]
    cameras = cam_rhs.shape[1]
    blocks = cameras // CAM_BLK
    points = pt_rhs.shape[1]
    chips = pts_size * grp_size // 2
    chunks = -(-blocks // PER)
    slots = -(-chunks // 16) * 8
    assert obs == blocks * 64 and slots <= chips and slots == 16 and points == 2048
    live = -(-obs // 128)
    groups = 2 * (-(-live // 16))

    def pad_obs(v):
        return jnp.pad(v, (0, 64 * 128 - obs)).reshape(64, 128)

    def vmem(*shape):
        return pltpu.VMEM(shape, F32)

    dma = pltpu.SemaphoreType.DMA
    anywhere = pl.BlockSpec(memory_space=pl.ANY)
    wide = live * 128
    camera_step, point_step, ratio = pl.pallas_call(
        functools.partial(body, chips, grp_size, chunks, slots, blocks, live, groups, obs),
        out_shape=(
            jax.ShapeDtypeStruct((9, cameras), F32),
            jax.ShapeDtypeStruct((3, points), F32),
            jax.ShapeDtypeStruct((1, 1), F32),
        ),
        in_specs=[VMEM] * 6 + [anywhere] * 2,
        out_specs=(VMEM, VMEM, VMEM),
        scratch_shapes=[
            vmem(18 * 64, 128), vmem(6 * 64, 128), vmem(9 * 16, 128), vmem(48, 128), vmem(16, 128),
            pltpu.VMEM((128, wide), BF16), pltpu.VMEM((128, wide), BF16), pltpu.VMEM((96, wide), BF16),
            vmem(3 * 64, 128), vmem(16 * 64, 128), vmem(48, 128), vmem(2 * slots * ROWS, 128),
            vmem(PER, 9, 9, 128), vmem(PER, 9, 128), vmem(ROWS, 128),
            vmem(slots, ROWS, 128), vmem(slots, ROWS, 128), vmem(chips, ROWS, 128), vmem(2 * slots * ROWS, 128),
            vmem(ROWS, 128), vmem(16, 128), vmem(16, 128), vmem(chips, 16, 128),
            dma((slots,)), dma((slots,)), dma((slots,)), dma((chips,)),
            dma((chips,)), dma((slots,)), dma((slots,)), dma((slots,)),
            dma((2 * PER,)), dma, dma, dma((chips,)), dma((chips,)),
        ],
        compiler_params=pltpu.CompilerParams(collective_id=0, has_side_effects=True),
        name="schur",
    )(cam_jac, pt_jac, pad_obs(cam_slot), pad_obs(obs_point), pt_inverse, pt_rhs, cam_inverse, cam_rhs)
    return camera_step, point_step, ratio.reshape(())


def solution(mesh):
    placed = (
        P(None, None, ("pts", "grp")),
        P(None, None, ("pts", "grp")),
        P(("pts", "grp")),
        P(("pts", "grp")),
        P(),
        P(None, None, ("pts", "grp")),
        P(),
        P(None, ("pts", "grp")),
    )
    return jax.shard_map(
        functools.partial(local, mesh.shape["pts"], mesh.shape["grp"]),
        mesh=mesh,
        in_specs=placed,
        out_specs=(P(), P(None, ("pts", "grp")), P()),
        check_vma=False,
    )
```

```python
import functools

import jax
import jax.numpy as jnp
from jax import lax
from jax.experimental import pallas as pl
from jax.experimental.pallas import tpu as pltpu
from jax.sharding import PartitionSpec as P

CAM_BLK = 128
TERMS = 3
PER = 4
ROWS = 40
MESH = pl.DeviceIdType.MESH
VMEM = pl.BlockSpec(memory_space=pltpu.VMEM)
F32 = jnp.float32
BF16 = jnp.bfloat16


def halves(v):
    top = v.astype(BF16)
    return top, (v - top.astype(F32)).astype(BF16)


def rows_of(group):
    return 16 * (group // 2) + group % 2


def prepare(
    obs, live, cj_in, pj_in, slot_in, point_in, pinv_in, prhs_in, cj, pj, slot, point, pinv, prhs, tail, right, hot
):
    begin = live // 8 * 8
    for ref, count in ((cj, 18), (pj, 6), (slot, 1), (point, 1)):
        for j in range(count):
            ref[j * 64 + begin : (j + 1) * 64, :] = jnp.zeros((64 - begin, 128), ref.dtype)
    tail[...] = jnp.zeros((16, 128), F32)
    for r in range(live):
        span = min(128, obs - r * 128)
        cols = slice(r * 128, r * 128 + span)
        for ref, out, count in ((cj_in, cj, 9), (pj_in, pj, 3)):
            for j in range(count):
                v = ref[j, :, cols]
                if span < 128:
                    tail[0:2, 0:span] = v
                    v = tail[0:2, :]
                out[pl.ds(j * 64 + r, 2, stride=count * 64), :] = v
        slot[r : r + 1, 0:span] = slot_in[0:1, cols]
        point[r : r + 1, 0:span] = point_in[0:1, cols]
    for s in range(16):
        cols = slice(s * 128, s * 128 + 128)
        prhs[pl.ds(s, 3, stride=16), :] = prhs_in[:, cols]
        for i in range(3):
            pinv[pl.ds(48 * i + s, 3, stride=16), :] = pinv_in[i, :, cols]
    low = lax.broadcasted_iota(jnp.int32, (128, 128), 0)
    for r in range(live):
        cols = slice(r * 128, (r + 1) * 128)
        right[:, cols] = jnp.where(low == (point[r : r + 1, :] & 127), 1.0, 0.0).astype(BF16)
        hot[:, cols] = jnp.where(low == slot[r : r + 1, :], 1.0, 0.0).astype(BF16)


def to_points(live, groups, vec, cj, pj, slot, point, quant, left, right):
    lane_low = lax.broadcasted_iota(jnp.int32, (8, 128), 1) < 64
    for group in range(groups):
        u, half = group // 2, group % 2
        row = rows_of(group)
        index = slot[pl.ds(row, 8, stride=2), :]
        proj = [None, None]
        for j in range(9):
            even = vec[pl.ds(8 * u * ROWS + (2 * half) * 9 + j, 8, stride=ROWS), :]
            odd = vec[pl.ds(8 * u * ROWS + (2 * half + 1) * 9 + j, 8, stride=ROWS), :]
            even = jnp.take_along_axis(even, index, axis=1, mode="promise_in_bounds")
            odd = jnp.take_along_axis(odd, index, axis=1, mode="promise_in_bounds")
            got = jnp.where(lane_low, even, odd)
            for a in range(2):
                part = cj[pl.ds((a * 9 + j) * 64 + row, 8, stride=2), :] * got
                proj[a] = part if proj[a] is None else proj[a] + part
        for i in range(3):
            quant[pl.ds(64 * i + row, 8, stride=2), :] = (
                pj[pl.ds(64 * i + row, 8, stride=2), :] * proj[0]
                + pj[pl.ds(64 * (3 + i) + row, 8, stride=2), :] * proj[1]
            )
    high = lax.broadcasted_iota(jnp.int32, (16, 128), 0)
    for r in range(live):
        cols = slice(r * 128, (r + 1) * 128)
        hit = high == (point[r : r + 1, :] >> 7)
        for i in range(3):
            v = jnp.where(hit, quant[64 * i + r : 64 * i + r + 1, :], 0.0)
            top, rest = halves(v)
            left[i * 16 : i * 16 + 16, cols] = top
            left[48 + i * 16 : 64 + i * 16, cols] = rest
    both = lax.dot_general(left[...], right[...], (((1,), (1,)), ((), ())), preferred_element_type=F32)
    return both[0:48] + both[48:96]


def point_solve(pinv, y):
    out = []
    for i in range(3):
        row = 48 * i
        out.append(
            pinv[row : row + 16] * y[0:16] + pinv[row + 16 : row + 32] * y[16:32] + pinv[row + 32 : row + 48] * y[32:48]
        )
    return jnp.concatenate(out, axis=0)


def pull_back(groups, z, cj, pj, point, pull):
    for group in range(groups):
        row = rows_of(group)
        where = point[pl.ds(row, 8, stride=2), :]
        low, high = where & 127, where >> 7
        got = [jnp.zeros((8, 128), F32)] * 3
        for s in range(16):
            hit = high == s
            for i in range(3):
                table = jnp.broadcast_to(z[16 * i + s : 16 * i + s + 1, :], (8, 128))
                cand = jnp.take_along_axis(table, low, axis=1, mode="promise_in_bounds")
                got[i] = jnp.where(hit, cand, got[i])
        proj = []
        for a in range(2):
            part = None
            for i in range(3):
                term = pj[pl.ds((3 * a + i) * 64 + row, 8, stride=2), :] * got[i]
                part = term if part is None else part + term
            proj.append(part)
        for j in range(9):
            pull[pl.ds(64 * j + row, 8, stride=2), :] = (
                cj[pl.ds(64 * j + row, 8, stride=2), :] * proj[0]
                + cj[pl.ds(64 * (9 + j) + row, 8, stride=2), :] * proj[1]
            )


def deposit(rows, hot, pull, out):
    lane_low = lax.broadcasted_iota(jnp.int32, (16, 128), 1) < 64
    for r in rows:
        v = pull[pl.ds(r, 16, stride=64), :]
        e_top, e_rest = halves(jnp.where(lane_low, v, 0.0))
        o_top, o_rest = halves(jnp.where(lane_low, 0.0, v))
        lhs = jnp.concatenate([e_top, e_rest, o_top, o_rest], axis=0)
        d = lax.dot_general(
            lhs, hot[:, r * 128 : r * 128 + 128], (((1,), (1,)), ((), ())), preferred_element_type=F32
        )
        base = (r // 2) * ROWS + (r % 2) * 18
        out[base : base + 9, :] = (d[0:16] + d[16:32])[0:9]
        out[base + 9 : base + 18, :] = (d[32:48] + d[48:64])[0:9]


def body(
    chips, grp_size, chunks, slots, blocks, live, groups, obs,
    cj_in, pj_in, slot_in, point_in, pinv_in, prhs_in, cinv, crhs,
    cam_out, pt_out, ratio_out,
    cj, pj, slot, point, pinv, prhs, tail, right, hot, left, quant, pull, zs, x, inv, rhs, kept,
    twin_buf, mine, inbox, result, tile, pair, tiles, left_tiles,
    a_s, a_r, b_s, b_r, c_s, c_r, d_s, d_r, load, p_s, p_r, q_s, q_r,
):
    pts, grp = lax.axis_index("pts"), lax.axis_index("grp")
    core = lax.rem(pts, 2)
    chip = (pts // 2) * grp_size + grp
    twin = (pts + 1 - 2 * core, grp)

    def at(other):
        return (2 * (other // grp_size) + core, lax.rem(other, grp_size))

    def around(k):
        return lax.rem(chip + k, chips)

    def loop(start, step):
        def run(k, carry):
            step(k)
            return carry

        lax.fori_loop(start, chips, run, 0)

    barrier = pltpu.get_barrier_semaphore()
    pl.semaphore_signal(barrier, inc=1, device_id=twin, device_id_type=MESH)
    loop(1, lambda k: pl.semaphore_signal(barrier, inc=1, device_id=at(around(k)), device_id_type=MESH))

    def number(c, t):
        return 2 * lax.rem(13 * t, slots) + c

    def owned(c, t):
        return jnp.logical_and(t < slots, number(c, t) < chunks)

    def owned_block(b):
        return jnp.logical_and(chip < slots, number(core, chip) * PER + b < blocks)

    def loads(b):
        cols = pl.ds(pl.multiple_of((number(core, chip) * PER + b) * 128, 128), 128)
        return (
            pltpu.make_async_copy(cinv.at[:, :, cols], inv.at[b], load.at[2 * b]),
            pltpu.make_async_copy(crhs.at[:, cols], rhs.at[b], load.at[2 * b + 1]),
        )

    for b in range(PER):
        @pl.when(owned_block(b))
        def _():
            for copy in loads(b):
                copy.start()

        @pl.when(jnp.logical_not(owned_block(b)))
        def _():
            inv[b] = jnp.zeros((9, 9, 128), F32)
            rhs[b] = jnp.zeros((9, 128), F32)

    prepare(
        obs, live, cj_in, pj_in, slot_in, point_in, pinv_in, prhs_in,
        cj, pj, slot, point, pinv, prhs, tail, right, hot,
    )
    x[...] = jnp.zeros_like(x)
    result[...] = jnp.zeros_like(result)
    kept[...] = jnp.zeros_like(kept)
    pull[pl.ds(9 * 64, 7 * 64), :] = jnp.zeros((7 * 64, 128), F32)
    zs[...] = prhs[...]
    for b in range(PER):
        @pl.when(owned_block(b))
        def _():
            for copy in loads(b):
                copy.wait()

    pl.semaphore_wait(barrier, chips)

    def chunk(c, t):
        return pl.ds(pl.multiple_of(number(c, t) * ROWS, 8), ROWS)

    def remote(src, dst, send, recv, device):
        return pltpu.make_async_remote_copy(
            src_ref=src, dst_ref=dst, send_sem=send, recv_sem=recv, device_id=device, device_id_type=MESH
        )

    def to_twin(t):
        return remote(x.at[chunk(1 - core, t)], twin_buf.at[t], a_s.at[t], a_r.at[t], twin)

    def to_owner(t):
        return remote(mine.at[t], inbox.at[chip], b_s.at[t], b_r.at[chip], at(t))

    def from_peer(t):
        return remote(mine.at[0], inbox.at[t], b_s.at[0], b_r.at[t], at(t))

    def spread(t):
        part = result.at[chunk(core, chip)]
        return remote(part, part, c_s.at[t], c_r.at[chip], at(t))

    def spread_in(t):
        part = result.at[chunk(core, t)]
        return remote(part, part, c_s.at[0], c_r.at[t], at(t))

    def pass_on(t):
        part = result.at[chunk(core, t)]
        return remote(part, part, d_s.at[t], d_r.at[t], twin)

    def pass_in(t):
        part = result.at[chunk(1 - core, t)]
        return remote(part, part, d_s.at[0], d_r.at[t], twin)

    early = -(-chunks // 4)

    def within(c, t, part):
        first = number(c, t) < 2 * early
        return jnp.logical_and(owned(c, t), first if part == 0 else jnp.logical_not(first))

    def start_twin(k, part):
        t = around(k)
        pl.when(within(1 - core, t, part))(lambda: to_twin(t).start())

    def reduce_pair(k, send, part):
        t = around(k)

        @pl.when(within(core, t, part))
        def _():
            to_twin(t).wait_recv()
            mine[t] = x[chunk(core, t), :] + twin_buf[t]
            if send:
                to_owner(t).start()

    def forward(k):
        t = around(chips - k)

        @pl.when(owned(core, t))
        def _():
            spread_in(t).wait_recv()
            pass_on(t).start()

    def finish(k):
        t = around(k)
        pl.when(owned(1 - core, t))(lambda: pass_in(t).wait_recv())

    def drain(k):
        t = around(k)
        pl.when(owned(1 - core, t))(lambda: to_twin(t).wait_send())
        pl.when(owned(core, t))(lambda: pass_on(t).wait_send())

    def drain_peers(k):
        t = around(k)
        pl.when(owned(core, t))(lambda: to_owner(t).wait_send())
        pl.when(owned(core, chip))(lambda: spread(t).wait_send())

    def exchange(index):
        for part in range(2):
            loop(1, lambda k: reduce_pair(k, True, part))
        for part in range(2):
            reduce_pair(0, False, part)

        @pl.when(owned(core, chip))
        def _():
            tile[...] = mine[chip]

            def gather(k):
                t = around(chips - k)
                from_peer(t).wait_recv()
                tile[...] += inbox[t]

            loop(1, gather)
            solved = []
            for b in range(PER):
                total = tile[9 * b : 9 * b + 9, :]
                total = jnp.where(index == 0, rhs[b] - total, total)
                piece = None
                for j in range(9):
                    term = inv[b, j] * total[j : j + 1, :]
                    piece = term if piece is None else piece + term
                solved.append(piece)
            solved = jnp.concatenate(solved + [jnp.zeros((ROWS - 9 * PER, 128), F32)], axis=0)
            step = kept[...] + solved
            kept[...] = step
            result[chunk(core, chip), :] = jnp.where(index == TERMS, step, solved)
            loop(1, lambda k: spread(around(k)).start())
            pass_on(chip).start()

        loop(1, forward)
        loop(0, finish)
        loop(0, drain)
        loop(1, drain_peers)

    def term(index, carry):
        solved = point_solve(pinv, zs[...])
        zs[...] = solved
        pull_back(groups, zs, cj, pj, point, pull)
        deposit(range(4 * early), hot, pull, x)
        loop(1, lambda k: start_twin(k, 0))
        start_twin(0, 0)
        deposit(range(4 * early, live), hot, pull, x)
        loop(1, lambda k: start_twin(k, 1))
        start_twin(0, 1)
        exchange(index)
        zs[...] = to_points(live, groups, result, cj, pj, slot, point, quant, left, right)
        return carry

    lax.fori_loop(0, TERMS + 1, term, 0)
    rhs_pts = prhs[...]
    resid = rhs_pts - zs[...]
    for row, vals in ((0, resid * resid), (1, rhs_pts * rhs_pts)):
        total = vals[0:8]
        for k in range(1, 6):
            total = total + vals[8 * k : 8 * k + 8]
        tiles[8 * row : 8 * row + 8, :] = total

    def swap():
        return remote(tiles, pair, p_s, p_r, twin)

    def share(t, slot_of):
        return remote(left_tiles.at[chip], left_tiles.at[slot_of], q_s.at[t], q_r.at[slot_of], at(t))

    swap().start()
    swap().wait_recv()
    left_tiles[chip] = tiles[...] + pair[...]
    loop(1, lambda k: share(around(k), chip).start())
    zs[...] = point_solve(pinv, resid)
    for s in range(16):
        pt_out[:, s * 128 : s * 128 + 128] = zs[pl.ds(s, 3, stride=16), :]
    for b in range(blocks):
        base = (b // PER) * ROWS + (b % PER) * 9
        cam_out[:, b * 128 : b * 128 + 128] = result[base : base + 9, :]

    def collect(k):
        t = around(k)
        share(t, t).wait_recv()

    loop(1, collect)
    total = left_tiles[0]
    for t in range(1, chips):
        total = total + left_tiles[t]
    ratio_out[...] = jnp.sqrt(jnp.sum(total[0:8], keepdims=True) / jnp.sum(total[8:16], keepdims=True))
    loop(1, lambda k: share(around(k), chip).wait_send())
    swap().wait_send()


def local(pts_size, grp_size, cam_jac, pt_jac, cam_slot, obs_point, cam_inverse, pt_inverse, cam_rhs, pt_rhs):
    obs = cam_slot.shape[0]
    cameras = cam_rhs.shape[1]
    blocks = cameras // CAM_BLK
    points = pt_rhs.shape[1]
    chips = pts_size * grp_size // 2
    chunks = -(-blocks // PER)
    slots = -(-chunks // 16) * 8
    assert obs == blocks * 64 and slots <= chips and slots == 16 and points == 2048
    live = -(-obs // 128)
    groups = 2 * (-(-live // 16))

    def vmem(*shape):
        return pltpu.VMEM(shape, F32)

    dma = pltpu.SemaphoreType.DMA
    anywhere = pl.BlockSpec(memory_space=pl.ANY)
    wide = live * 128
    camera_step, point_step, ratio = pl.pallas_call(
        functools.partial(body, chips, grp_size, chunks, slots, blocks, live, groups, obs),
        out_shape=(
            jax.ShapeDtypeStruct((9, cameras), F32),
            jax.ShapeDtypeStruct((3, points), F32),
            jax.ShapeDtypeStruct((1, 1), F32),
        ),
        in_specs=[VMEM] * 6 + [anywhere] * 2,
        out_specs=(VMEM, VMEM, VMEM),
        scratch_shapes=[
            vmem(18 * 64, 128), vmem(6 * 64, 128),
            pltpu.VMEM((64, 128), jnp.int32), pltpu.VMEM((64, 128), jnp.int32), vmem(9 * 16, 128), vmem(48, 128), vmem(16, 128),
            pltpu.VMEM((128, wide), BF16), pltpu.VMEM((128, wide), BF16), pltpu.VMEM((96, wide), BF16),
            vmem(3 * 64, 128), vmem(16 * 64, 128), vmem(48, 128), vmem(2 * slots * ROWS, 128),
            vmem(PER, 9, 9, 128), vmem(PER, 9, 128), vmem(ROWS, 128),
            vmem(slots, ROWS, 128), vmem(slots, ROWS, 128), vmem(chips, ROWS, 128), vmem(2 * slots * ROWS, 128),
            vmem(ROWS, 128), vmem(16, 128), vmem(16, 128), vmem(chips, 16, 128),
            dma((slots,)), dma((slots,)), dma((slots,)), dma((chips,)),
            dma((chips,)), dma((slots,)), dma((slots,)), dma((slots,)),
            dma((2 * PER,)), dma, dma, dma((chips,)), dma((chips,)),
        ],
        compiler_params=pltpu.CompilerParams(collective_id=0, has_side_effects=True),
        name="schur",
    )(
        jnp.transpose(cam_jac, (1, 0, 2)), jnp.transpose(pt_jac, (1, 0, 2)),
        cam_slot.reshape(1, obs), obs_point.reshape(1, obs), pt_inverse, pt_rhs, cam_inverse, cam_rhs,
    )
    return camera_step, point_step, ratio.reshape(())


def solution(mesh):
    placed = (
        P(None, None, ("pts", "grp")),
        P(None, None, ("pts", "grp")),
        P(("pts", "grp")),
        P(("pts", "grp")),
        P(),
        P(None, None, ("pts", "grp")),
        P(),
        P(None, ("pts", "grp")),
    )
    return jax.shard_map(
        functools.partial(local, mesh.shape["pts"], mesh.shape["grp"]),
        mesh=mesh,
        in_specs=placed,
        out_specs=(P(), P(None, ("pts", "grp")), P()),
        check_vma=False,
    )
```
